32 devices in a mesh: rep: 4 (over x, core), shard: 8 (over z, y).
Axes of the slice: x: 2, y: 2, z: 4, core: 2. Of those that a mesh axis runs over, the one named last changes fastest.
Arguments:
- grads: float32 [4, 8, 16, 128, 128], P('rep', 'shard'), may hold values from -24 to 24
- counts: int32 [4, 8, 16, 128], P('rep', 'shard'), may hold values from 0 to 5
- block_owner: int32 [4, 8, 16, 1], P('rep', 'shard'), may hold values from 0 to 7; in each aligned block of 16 rows (0 to 15, 16 to 31, ..., all dimensions but the last counted through in order) at most 4 rows name the same one
- block_local: int32 [4, 8, 16], P('rep', 'shard'), may hold values from 0 to 63
Outputs:
- clipped: float32 [512, 128, 128], P('shard', 'rep')
The draws below stay inside these ranges and needn't reach their ends.
Inputs may be any that keep to these rules, and one draw needn't show every extreme that they name: `block_owner`: among the 16 blocks of one device no owner is named more than 4 times, a bound that some block reaches.
All inputs are finite; a program needn't handle non-finite values.
Results may differ from the reference program's by a relative error of at most 0.0003.
Values sent between devices are 32-bit elements; how exact they have to be, the bound alone decides.
A program may use at most 128 MiB of HBM per device.

```python
import math
import jax
import jax.numpy as jnp
import numpy as np
from jax import lax

D = 128
BR = 128
BLK_SHARD = 64
KB = 16
CAP = 4
N_REP = 4
N_SHARD = 8


def with_ends(result, stream_key, smallest, largest):
    longest = result.shape.index(max(result.shape))
    spots = []
    for shift in (0, 1):
        where = [jax.random.randint(jax.random.fold_in(stream_key, axis), (), 0, length) for axis, length in enumerate(result.shape)]
        where[longest] = (where[longest] + shift) % result.shape[longest]
        spots.append(tuple(where))
    return result.at[spots[0]].set(smallest).at[spots[1]].set(largest)


def block_scale(own_key, shape, shards, least, top_value):
    def one(axis_at, parts):
        draws = jax.random.uniform(jax.random.fold_in(jax.random.fold_in(own_key, 6), axis_at), (parts,), jnp.float32, least / len(shards), top_value / len(shards))
        return jnp.repeat(jnp.exp(draws), shape[axis_at] // parts).reshape((-1,) + (1,) * (len(shape) - axis_at - 1))

    level = one(*shards[0])
    for cut in shards[1:]:
        level = level * one(*cut)
    return level


def rank_table(amount, slope):
    weights = [(1 << 20) // math.isqrt(standing ** slope) + 1 for standing in range(1, amount + 1)]
    spread = 1 + sum(weights) // (1 << 30)
    return np.cumsum(np.array([max(1, weight // spread) for weight in weights]))


def skewed_ids(rng, dims, amount, skew):
    grid = rank_table(amount, skew)
    lot = jax.random.randint(jax.random.fold_in(rng, 1), dims, 0, int(grid[amount - 1]))
    grade = jnp.searchsorted(jnp.asarray(grid, jnp.int32), lot, side="right")
    return jax.random.permutation(jax.random.fold_in(rng, 2), amount)[grade].astype(jnp.int32)


def shared_out(stream_key, own, number, rows, amount, top, bound, skew):
    sequence = jax.random.permutation(stream_key, amount)
    heavy_load, common = portions_of(amount, rows * top, bound, skew, True), portions_of(amount, rows * top, bound, skew, False)
    places = jnp.arange(amount)

    def named(lengths, rotation):
        used = int((lengths > 0).sum())
        fixed = max(1, used // 4)
        shifted = fixed + (places - fixed + rotation * (used - fixed)) % max(1, amount - fixed)
        return jnp.zeros((amount,), jnp.int32).at[sequence[jnp.where(places < fixed, places, shifted)]].set(jnp.asarray(lengths, jnp.int32))

    lengths = jnp.where(number % 4 == 0, named(heavy_load, number // 4), named(common, number - number // 4 - 1))
    mixed = jax.random.permutation(jax.random.fold_in(own, 3), amount)
    source_of, taker = mixed[0:amount // 2 * 2:2], mixed[1:amount // 2 * 2:2]
    slack = jnp.minimum(lengths[source_of] - 1, bound - lengths[taker]) // 2
    slack = jnp.where((source_of == sequence[0]) | (taker == sequence[0]) | (lengths[taker] == 0), 0, jnp.maximum(slack, 0))
    shifted = jax.random.randint(jax.random.fold_in(own, 4), (amount // 2,), 0, 1 << 20) % (slack + 1)
    lengths = lengths.at[source_of].add(-shifted).at[taker].add(shifted)
    items = jnp.searchsorted(jnp.cumsum(lengths), jnp.arange(rows * top), side="right").astype(jnp.int32)
    listing = items.reshape(top, rows).T
    listing = listing[jax.random.permutation(jax.random.fold_in(own, 1), rows)]
    rotation = jax.random.randint(jax.random.fold_in(own, 2), (rows, 1), 0, top)
    return jnp.take_along_axis(listing, (jnp.arange(top)[None, :] + rotation) % top, axis=1)


def portions_of(amount, total, most, lean, full):
    portions = [(1 << 20) // math.isqrt(grade ** lean) + 1 for grade in range(1, amount + 1)]
    largest = most if full else min(most, max(-(-total // amount), total * portions[0] // sum(portions)))
    least = 1 if total - largest >= amount - 1 else 0
    holding, rest = [largest] + [least] * (amount - 1), total - largest - least * (amount - 1)
    while rest > 0:
        free = [i for i in range(1, amount) if holding[i] < largest] or [i for i in range(1, amount) if holding[i] < most]
        mass, left = sum([portions[i] for i in free]), rest
        for i in free:
            addition = min(most - holding[i], max(1, left * portions[i] // mass), rest)
            holding[i] = holding[i] + addition
            rest = rest - addition
    return np.array(holding)


def noise(stream_key, extent, deviation, most, split=(), held_as=jnp.bfloat16):
    result = jax.random.normal(stream_key, extent, jnp.float32) * deviation
    if len(split) > 0:
        result = block_scale(stream_key, extent, split, -0.22, 0.18) * result
    return jnp.clip(result, min=-most, max=most).astype(held_as)


def setup_inputs(seed: int = 0) -> dict:
    arg_keys = jax.random.split(jax.random.key(seed), 5)
    grads = noise(arg_keys[0], (N_REP, N_SHARD, KB, BR, D), 4.0, 24.0, ((0, 4), (1, 8)), jnp.float32)
    counts = with_ends(jax.random.randint(arg_keys[1], (N_REP, N_SHARD, KB, BR), 0, 6), jax.random.fold_in(arg_keys[1], 1), 0, 5).astype(jnp.int32)
    block_owner_keys = jax.random.split(jax.random.fold_in(arg_keys[2], 1), N_REP * N_SHARD * KB // KB)
    block_owner_turns = jax.random.permutation(jax.random.fold_in(arg_keys[2], 3), N_REP * N_SHARD * KB // KB)
    block_owner = jax.vmap(lambda own, number: shared_out(jax.random.fold_in(arg_keys[2], 2), own, number, KB, N_SHARD, 1, CAP, 2))(block_owner_keys, block_owner_turns).reshape((N_REP, N_SHARD, KB, 1))
    block_local = with_ends(skewed_ids(arg_keys[3], (N_REP, N_SHARD, KB), BLK_SHARD, 2), jax.random.fold_in(arg_keys[3], 3), 0, BLK_SHARD - 1).astype(jnp.int32)
    return dict(grads=grads, counts=counts, block_owner=block_owner, block_local=block_local)


def reference(grads, counts, block_owner, block_local):
    total_blocks = BLK_SHARD * N_SHARD
    block_ids = (block_owner[..., 0] * BLK_SHARD + block_local).astype(jnp.int32)

    def add_replica(carry, items):
        sums, totals = carry
        blocks, cnts, ids = items
        blocks = blocks.reshape(-1, BR, D)
        cnts = cnts.reshape(-1, BR)
        ids = ids.reshape(-1)
        masked = jnp.where(cnts[..., None] > 0, blocks, jnp.float32(0.0))
        sums = sums + jax.ops.segment_sum(masked, ids, total_blocks)
        totals = totals + jax.ops.segment_sum(cnts.astype(jnp.float32), ids, total_blocks)
        return ((sums, totals), None)
    start = (jnp.zeros((total_blocks, BR, D), jnp.float32), jnp.zeros((total_blocks, BR), jnp.float32))
    (sums, totals), unused = lax.scan(add_replica, start, (grads, counts, block_ids))
    mean = sums / jnp.maximum(totals, jnp.float32(1.0))[..., None]
    norm2 = jnp.sum(mean * mean)
    limit = jnp.float32(0.2 * math.sqrt(total_blocks * BR * D))
    scale = jnp.minimum(jnp.float32(1.0), limit / jnp.sqrt(norm2 + jnp.float32(1e-06)))
    return mean * scale
```

```python
import functools
import math

import jax
import jax.numpy as jnp
from jax import lax
from jax.experimental import pallas as pl
from jax.experimental.pallas import tpu as pltpu
from jax.sharding import PartitionSpec as P

BLK_SHARD = 64
CAP = 4
META = 8
CHUNK = 8


def xor(a, b, n):
    out = jnp.int32(0)
    bit = 1
    while bit < n:
        x = lax.rem(lax.div(a, jnp.int32(bit)), jnp.int32(2))
        y = lax.rem(lax.div(b, jnp.int32(bit)), jnp.int32(2))
        out = out + bit * (x + y - 2 * x * y)
        bit *= 2
    return out


def kernel(
    nrep, nshard, limit,
    own_ref, loc_ref, cnt_ref, grads_ref, out_ref,
    masked, stg, recv, acc, tot, invt, part, norms,
    send_sem, recv_sem, nsend_sem, nrecv_sem,
):
    nblocks, rows, width = grads_ref.shape
    prow = rows // nrep
    peers = nrep * nshard
    rep = lax.axis_index("rep")
    shard = lax.axis_index("shard")

    def peer(k):
        ks, kr = lax.div(k, jnp.int32(nrep)), lax.rem(k, jnp.int32(nrep))
        return (xor(rep, kr, nrep), xor(shard, ks, nshard))

    barrier = pltpu.get_barrier_semaphore()

    def greet(i, carry):
        pl.semaphore_signal(
            barrier, inc=1, device_id=peer(i), device_id_type=pl.DeviceIdType.MESH
        )
        return carry

    lax.fori_loop(1, peers, greet, 0)

    cntf = cnt_ref[...].astype(jnp.float32)
    cols = cntf.T
    for b in range(nblocks):
        masked[b] = jnp.where(cols[:, b : b + 1] > 0, grads_ref[b], jnp.float32(0.0))

    def pack(i, carry):
        ks = nshard - 1 - i
        owner = xor(shard, ks, nshard)

        def scan(b, state):
            seen, src, ids = state
            hit = own_ref[b] == owner
            loc = loc_ref[b]
            take = [hit & (seen == c) for c in range(CAP)]
            src = tuple(jnp.where(take[c], b, src[c]) for c in range(CAP))
            ids = tuple(jnp.where(take[c], loc, ids[c]) for c in range(CAP))
            return (seen + hit.astype(jnp.int32), src, ids)

        zero, none = jnp.int32(0), jnp.int32(-1)
        unused, src, ids = lax.fori_loop(
            0, nblocks, scan, (zero, (zero,) * CAP, (none,) * CAP), unroll=16
        )
        for c in range(CAP):
            line = cnt_ref[pl.ds(src[c], 1), :].astype(jnp.float32)
            name = jnp.full((1, width), ids[c], jnp.int32).astype(jnp.float32)
            for kr in range(nrep):
                k = ks * nrep + kr
                first = pl.multiple_of(xor(rep, jnp.int32(kr), nrep) * prow, prow)
                stg[k, pl.ds(META + c * prow, prow), :] = masked[src[c], pl.ds(first, prow), :]
                stg[k, pl.ds(c, 1), :] = line
                stg[k, pl.ds(CAP + c, 1), :] = name
        return carry

    lax.fori_loop(0, nshard, pack, 0)
    acc[...] = jnp.zeros_like(acc)
    tot[...] = jnp.zeros_like(tot)

    pl.semaphore_wait(barrier, peers - 1)

    def message(k):
        return pltpu.make_async_remote_copy(
            src_ref=stg.at[k],
            dst_ref=recv.at[k],
            send_sem=send_sem.at[k],
            recv_sem=recv_sem.at[k],
            device_id=peer(k),
            device_id_type=pl.DeviceIdType.MESH,
        )

    def send(i, carry):
        message(peers - 1 - i).start()
        return carry

    lax.fori_loop(0, peers - 1, send, 0)

    def add(source, k):
        names = [source[k, pl.ds(CAP + c, 1), :] for c in range(CAP)]
        lines = [source[k, pl.ds(c, 1), :] for c in range(CAP)]
        block = lax.broadcasted_iota(jnp.int32, (BLK_SHARD, width), 0).astype(jnp.float32)
        total = tot[...]
        for c in range(CAP):
            total = total + jnp.where(block == names[c], lines[c], jnp.float32(0.0))
        tot[...] = total

        def some(j, carry):
            at = pl.multiple_of(j * CHUNK, CHUNK)
            value = [acc[at + t] for t in range(CHUNK)]
            for c in range(CAP):
                held = source[k, pl.ds(META + c * prow, prow), :]
                name = jnp.broadcast_to(names[c], (prow, width))
                for t in range(CHUNK):
                    hot = name == (at + t).astype(jnp.float32)
                    value[t] = value[t] + jnp.where(hot, held, jnp.float32(0.0))
            for t in range(CHUNK):
                acc[at + t] = value[t]
            return carry

        lax.fori_loop(0, BLK_SHARD // CHUNK, some, 0)

    add(stg, 0)

    def take(k):
        message(k).wait_recv()
        add(recv, k)

    def near(k, carry):
        take(k)
        return carry

    def far(i, carry):
        take(peers - 1 - i)
        return carry

    lax.fori_loop(1, peers // 2, near, 0)
    lax.fori_loop(0, peers - peers // 2, far, 0)

    def sent(k, carry):
        message(k).wait_send()
        return carry

    lax.fori_loop(1, peers, sent, 0)

    invt[...] = (jnp.float32(1.0) / jnp.maximum(tot[...], jnp.float32(1.0))).T
    inv = invt[pl.ds(pl.multiple_of(rep * prow, prow), prow), :]
    square = jnp.zeros((prow, width), jnp.float32)
    for t in range(BLK_SHARD):
        mean = acc[t] * inv[:, t : t + 1]
        acc[t] = mean
        square = square + mean * mean
    part[...] = jnp.sum(square.reshape(prow // 8, 8, width), axis=0)

    def norm(k):
        return pltpu.make_async_remote_copy(
            src_ref=part,
            dst_ref=norms.at[k],
            send_sem=nsend_sem.at[k],
            recv_sem=nrecv_sem.at[k],
            device_id=peer(k),
            device_id_type=pl.DeviceIdType.MESH,
        )

    def nsend(i, carry):
        norm(peers - 1 - i).start()
        return carry

    lax.fori_loop(0, peers - 1, nsend, 0)

    def ntake(k, total):
        norm(k).wait_recv()
        return total + norms[k]

    total = lax.fori_loop(1, peers, ntake, part[...])
    norm2 = jnp.sum(jnp.sum(total, axis=0, keepdims=True), axis=1, keepdims=True)
    scale = jnp.minimum(jnp.float32(1.0), limit / jnp.sqrt(norm2 + jnp.float32(1e-06)))
    for t in range(BLK_SHARD):
        out_ref[t] = acc[t] * scale

    def nsent(k, carry):
        norm(k).wait_send()
        return carry

    lax.fori_loop(1, peers, nsent, 0)


def local(nrep, nshard, grads, counts, block_owner, block_local):
    nblocks, rows, width = grads.shape[2:]
    peers = nrep * nshard
    prow = rows // nrep
    limit = math.sqrt(BLK_SHARD * nshard * rows * width) * 0.2
    body = functools.partial(kernel, nrep, nshard, limit)
    smem = pl.BlockSpec(memory_space=pltpu.SMEM)
    vmem = pl.BlockSpec(memory_space=pltpu.VMEM)
    size = META + CAP * prow
    return pl.pallas_call(
        body,
        out_shape=jax.ShapeDtypeStruct((BLK_SHARD, prow, width), jnp.float32),
        in_specs=[smem, smem, vmem, vmem],
        out_specs=vmem,
        scratch_shapes=[
            pltpu.VMEM((nblocks, rows, width), jnp.float32),
            pltpu.VMEM((peers, size, width), jnp.float32),
            pltpu.VMEM((peers, size, width), jnp.float32),
            pltpu.VMEM((BLK_SHARD, prow, width), jnp.float32),
            pltpu.VMEM((BLK_SHARD, width), jnp.float32),
            pltpu.VMEM((width, BLK_SHARD), jnp.float32),
            pltpu.VMEM((8, width), jnp.float32),
            pltpu.VMEM((peers, 8, width), jnp.float32),
            pltpu.SemaphoreType.DMA((peers,)),
            pltpu.SemaphoreType.DMA((peers,)),
            pltpu.SemaphoreType.DMA((peers,)),
            pltpu.SemaphoreType.DMA((peers,)),
        ],
        compiler_params=pltpu.CompilerParams(collective_id=0, has_side_effects=True),
        name="exchange",
    )(
        block_owner.reshape(nblocks),
        block_local.reshape(nblocks),
        counts.reshape(nblocks, rows),
        grads.reshape(nblocks, rows, width),
    )


def solution(mesh):
    body = functools.partial(local, mesh.shape["rep"], mesh.shape["shard"])
    return jax.shard_map(
        body,
        mesh=mesh,
        in_specs=(
            P("rep", "shard", None, None, None),
            P("rep", "shard", None, None),
            P("rep", "shard", None, None),
            P("rep", "shard", None),
        ),
        out_specs=P("shard", "rep", None),
        check_vma=False,
    )
```

```python
import functools
import math

import jax
import jax.numpy as jnp
from jax import lax
from jax.experimental import pallas as pl
from jax.experimental.pallas import tpu as pltpu
from jax.sharding import PartitionSpec as P

BLK_SHARD = 64
CAP = 4
META = 2
CHUNK = 8


def xor(a, b, n):
    out = jnp.int32(0)
    bit = 1
    while bit < n:
        x = lax.rem(lax.div(a, jnp.int32(bit)), jnp.int32(2))
        y = lax.rem(lax.div(b, jnp.int32(bit)), jnp.int32(2))
        out = out + bit * (x + y - 2 * x * y)
        bit *= 2
    return out


def kernel(
    nrep, nshard, limit,
    own_ref, loc_ref, cnt_ref, grads_ref, out_ref, scale_ref,
    masked, stg, recv, acc, tot, part, norms,
    out_sem, send_sem, recv_sem, nsend_sem, nrecv_sem,
):
    nblocks, rows, width = grads_ref.shape
    prow = rows // nrep
    peers = nrep * nshard
    size = CAP * prow + META
    rep = lax.axis_index("rep")
    shard = lax.axis_index("shard")

    def peer(k):
        ks, kr = lax.div(k, jnp.int32(nrep)), lax.rem(k, jnp.int32(nrep))
        return (xor(rep, kr, nrep), xor(shard, ks, nshard))

    barrier = pltpu.get_barrier_semaphore()

    def greet(i, carry):
        pl.semaphore_signal(
            barrier, inc=1, device_id=peer(i), device_id_type=pl.DeviceIdType.MESH
        )
        return carry

    lax.fori_loop(1, peers, greet, 0)

    cntf = cnt_ref[...].astype(jnp.float32)
    cols = cntf.T
    for b in range(nblocks):
        masked[b] = jnp.where(cols[:, b : b + 1] > 0, grads_ref[b], jnp.float32(0.0))

    def order(i):
        far, near = lax.div(i, jnp.int32(2)), lax.rem(i, jnp.int32(2))
        return nshard - 1 - far - near * (nshard // 2)

    def pack(i):
        ks = order(i)
        owner = xor(shard, ks, nshard)

        def scan(b, state):
            seen, src, ids = state
            hit = own_ref[b] == owner
            loc = loc_ref[b]
            take = [hit & (seen == c) for c in range(CAP)]
            src = tuple(jnp.where(take[c], b, src[c]) for c in range(CAP))
            ids = tuple(jnp.where(take[c], loc, ids[c]) for c in range(CAP))
            return (seen + hit.astype(jnp.int32), src, ids)

        zero, none = jnp.int32(0), jnp.int32(-1)
        unused, src, ids = lax.fori_loop(
            0, nblocks, scan, (zero, (zero,) * CAP, (none,) * CAP), unroll=16
        )
        lane = lax.broadcasted_iota(jnp.int32, (1, width), 1)
        name = jnp.full((1, width), -1, jnp.int32)
        for c in range(CAP):
            name = jnp.where((lane >= c * prow) & (lane < (c + 1) * prow), ids[c], name)
        name = name.astype(jnp.float32)
        lines = [cnt_ref[pl.ds(src[c], 1), :].astype(jnp.float32) for c in range(CAP)]
        for p in range(nrep):
            k = ks * nrep + xor(rep, jnp.int32(p), nrep)
            line = jnp.zeros((1, width), jnp.float32)
            for c in range(CAP):
                stg[k, pl.ds(c * prow, prow), :] = masked[src[c], pl.ds(p * prow, prow), :]
                turned = pltpu.roll(lines[c], (c - p) * prow % width, 1)
                line = jnp.where((lane >= c * prow) & (lane < (c + 1) * prow), turned, line)
            stg[k, pl.ds(CAP * prow, 1), :] = line
            stg[k, pl.ds(CAP * prow + 1, 1), :] = name

    def message(k):
        return pltpu.make_async_remote_copy(
            src_ref=stg.at[k, pl.ds(0, size)],
            dst_ref=recv.at[k, pl.ds(0, size)],
            send_sem=send_sem.at[k],
            recv_sem=recv_sem.at[k],
            device_id=peer(k),
            device_id_type=pl.DeviceIdType.MESH,
        )

    def send(i, first):
        for kr in range(nrep - 1, first - 1, -1):
            message(order(i) * nrep + kr).start()

    pack(jnp.int32(0))
    pl.semaphore_wait(barrier, peers - 1)

    def step(i, carry):
        pack(i)
        send(i - 1, 0)
        return carry

    lax.fori_loop(1, nshard, step, 0)
    send(jnp.int32(nshard - 1), 1)
    acc[...] = jnp.zeros_like(acc)
    tot[...] = jnp.zeros_like(tot)

    def add(source, k):
        line = source[k, pl.ds(CAP * prow, 1), :]
        name = source[k, pl.ds(CAP * prow + 1, 1), :]
        names = [jnp.broadcast_to(name[:, c * prow : c * prow + 1], (1, width)) for c in range(CAP)]
        block = lax.broadcasted_iota(jnp.int32, (BLK_SHARD, width), 0).astype(jnp.float32)
        tot[...] = tot[...] + jnp.where(block == name, line, jnp.float32(0.0))

        def some(j, carry):
            at = pl.multiple_of(j * CHUNK, CHUNK)
            value = [acc[at + t] for t in range(CHUNK)]
            for c in range(CAP):
                held = source[k, pl.ds(c * prow, prow), :]
                name = jnp.broadcast_to(names[c], (prow, width))
                for t in range(CHUNK):
                    hot = name == (at + t).astype(jnp.float32)
                    value[t] = value[t] + jnp.where(hot, held, jnp.float32(0.0))
            for t in range(CHUNK):
                acc[at + t] = value[t]
            return carry

        lax.fori_loop(0, BLK_SHARD // CHUNK, some, 0)

    add(stg, 0)

    def take(k):
        message(k).wait_recv()
        add(recv, k)

    def group(h, carry):
        for near in (1, 0):
            ks = order(2 * h + near)
            for kr in range(nrep - 1, -1, -1):
                k = ks * nrep + kr
                if near and kr == 0:
                    pl.when(k > 0)(functools.partial(take, k))
                else:
                    take(k)
        return carry

    lax.fori_loop(0, nshard // 2, group, 0)

    def sent(k, carry):
        message(k).wait_send()
        return carry

    lax.fori_loop(1, peers, sent, 0)

    total = tot[...]
    for c in range(1, CAP):
        total = total + pltpu.roll(tot[...], -c * prow % width, 1)
    inv = (jnp.float32(1.0) / jnp.maximum(total, jnp.float32(1.0))).T[:prow, :]
    square = jnp.zeros((prow, width), jnp.float32)
    for t in range(BLK_SHARD):
        mean = acc[t] * inv[:, t : t + 1]
        acc[t] = mean
        square = square + mean * mean
    mean_copy = pltpu.make_async_copy(acc, out_ref, out_sem)
    mean_copy.start()
    part[...] = jnp.sum(square.reshape(prow // 8, 8, width), axis=0)

    def norm(k):
        return pltpu.make_async_remote_copy(
            src_ref=part,
            dst_ref=norms.at[k],
            send_sem=nsend_sem.at[k],
            recv_sem=nrecv_sem.at[k],
            device_id=peer(k),
            device_id_type=pl.DeviceIdType.MESH,
        )

    def nsend(i, carry):
        norm(peers - 1 - i).start()
        return carry

    lax.fori_loop(0, peers - 1, nsend, 0)

    def ntake(k, total):
        norm(k).wait_recv()
        return total + norms[k]

    total = lax.fori_loop(1, peers, ntake, part[...])
    norm2 = jnp.sum(jnp.sum(total, axis=0, keepdims=True), axis=1, keepdims=True)
    scale = jnp.minimum(jnp.float32(1.0), limit / jnp.sqrt(norm2 + jnp.float32(1e-06)))
    scale_ref[...] = scale
    mean_copy.wait()

    def nsent(k, carry):
        norm(k).wait_send()
        return carry

    lax.fori_loop(1, peers, nsent, 0)


def local(nrep, nshard, grads, counts, block_owner, block_local):
    nblocks, rows, width = grads.shape[2:]
    peers = nrep * nshard
    prow = rows // nrep
    limit = math.sqrt(BLK_SHARD * nshard * rows * width) * 0.2
    body = functools.partial(kernel, nrep, nshard, limit)
    smem = pl.BlockSpec(memory_space=pltpu.SMEM)
    vmem = pl.BlockSpec(memory_space=pltpu.VMEM)
    size = -(-(META + CAP * prow) // 8) * 8
    mean, scale = pl.pallas_call(
        body,
        out_shape=(
            jax.ShapeDtypeStruct((BLK_SHARD, prow, width), jnp.float32),
            jax.ShapeDtypeStruct((1, 1), jnp.float32),
        ),
        in_specs=[smem, smem, vmem, vmem],
        out_specs=(pl.BlockSpec(memory_space=pl.ANY), vmem),
        scratch_shapes=[
            pltpu.VMEM((nblocks, rows, width), jnp.float32),
            pltpu.VMEM((peers, size, width), jnp.float32),
            pltpu.VMEM((peers, size, width), jnp.float32),
            pltpu.VMEM((BLK_SHARD, prow, width), jnp.float32),
            pltpu.VMEM((BLK_SHARD, width), jnp.float32),
            pltpu.VMEM((8, width), jnp.float32),
            pltpu.VMEM((peers, 8, width), jnp.float32),
            pltpu.SemaphoreType.DMA,
            pltpu.SemaphoreType.DMA((peers,)),
            pltpu.SemaphoreType.DMA((peers,)),
            pltpu.SemaphoreType.DMA((peers,)),
            pltpu.SemaphoreType.DMA((peers,)),
        ],
        compiler_params=pltpu.CompilerParams(collective_id=0, has_side_effects=True),
        name="exchange",
    )(
        block_owner.reshape(nblocks),
        block_local.reshape(nblocks),
        counts.reshape(nblocks, rows),
        grads.reshape(nblocks, rows, width),
    )
    return mean * scale.reshape(())


def solution(mesh):
    body = functools.partial(local, mesh.shape["rep"], mesh.shape["shard"])
    return jax.shard_map(
        body,
        mesh=mesh,
        in_specs=(
            P("rep", "shard", None, None, None),
            P("rep", "shard", None, None),
            P("rep", "shard", None, None),
            P("rep", "shard", None),
        ),
        out_specs=P("shard", "rep", None),
        check_vma=False,
    )
```

```python
import functools
import math

import jax
import jax.numpy as jnp
from jax import lax
from jax.experimental import pallas as pl
from jax.experimental.pallas import tpu as pltpu
from jax.sharding import PartitionSpec as P

BLK_SHARD = 64
CAP = 4
META = 8
CHUNK = 8


def xor(a, b, n):
    out = jnp.int32(0)
    bit = 1
    while bit < n:
        x = lax.rem(lax.div(a, jnp.int32(bit)), jnp.int32(2))
        y = lax.rem(lax.div(b, jnp.int32(bit)), jnp.int32(2))
        out = out + bit * (x + y - 2 * x * y)
        bit *= 2
    return out


def kernel(
    nrep, nshard, limit,
    own_ref, loc_ref, cnt_ref, grads_ref, out_ref,
    masked, stg, recv, acc, tot, invt, part, norms,
    send_sem, recv_sem, nsend_sem, nrecv_sem,
):
    nblocks, rows, width = grads_ref.shape
    prow = rows // nrep
    peers = nrep * nshard
    rep = lax.axis_index("rep")
    shard = lax.axis_index("shard")

    def peer(k):
        ks, kr = lax.div(k, jnp.int32(nrep)), lax.rem(k, jnp.int32(nrep))
        return (xor(rep, kr, nrep), xor(shard, ks, nshard))

    barrier = pltpu.get_barrier_semaphore()

    def greet(i, carry):
        pl.semaphore_signal(
            barrier, inc=1, device_id=peer(i), device_id_type=pl.DeviceIdType.MESH
        )
        return carry

    lax.fori_loop(1, peers, greet, 0)

    cntf = cnt_ref[...].astype(jnp.float32)
    cols = cntf.T
    for b in range(nblocks):
        masked[b] = jnp.where(cols[:, b : b + 1] > 0, grads_ref[b], jnp.float32(0.0))

    def pack(i, carry):
        ks = nshard - 1 - i
        owner = xor(shard, ks, nshard)

        def scan(b, state):
            seen, src, ids = state
            hit = own_ref[b] == owner
            loc = loc_ref[b]
            take = [hit & (seen == c) for c in range(CAP)]
            src = tuple(jnp.where(take[c], b, src[c]) for c in range(CAP))
            ids = tuple(jnp.where(take[c], loc, ids[c]) for c in range(CAP))
            return (seen + hit.astype(jnp.int32), src, ids)

        zero, none = jnp.int32(0), jnp.int32(-1)
        unused, src, ids = lax.fori_loop(
            0, nblocks, scan, (zero, (zero,) * CAP, (none,) * CAP), unroll=16
        )
        for c in range(CAP):
            line = cnt_ref[pl.ds(src[c], 1), :].astype(jnp.float32)
            name = jnp.full((1, width), ids[c], jnp.int32).astype(jnp.float32)
            for kr in range(nrep):
                k = ks * nrep + kr
                first = pl.multiple_of(xor(rep, jnp.int32(kr), nrep) * prow, prow)
                stg[k, pl.ds(META + c * prow, prow), :] = masked[src[c], pl.ds(first, prow), :]
                stg[k, pl.ds(c, 1), :] = line
                stg[k, pl.ds(CAP + c, 1), :] = name
        return carry

    lax.fori_loop(0, nshard, pack, 0)
    acc[...] = jnp.zeros_like(acc)
    tot[...] = jnp.zeros_like(tot)

    pl.semaphore_wait(barrier, peers - 1)

    def message(k):
        return pltpu.make_async_remote_copy(
            src_ref=stg.at[k],
            dst_ref=recv.at[k],
            send_sem=send_sem.at[k],
            recv_sem=recv_sem.at[k],
            device_id=peer(k),
            device_id_type=pl.DeviceIdType.MESH,
        )

    def send(i, carry):
        far, near = lax.div(i, jnp.int32(2)), lax.rem(i, jnp.int32(2))
        message(peers - 1 - far - near * (peers // 2)).start()
        return carry

    lax.fori_loop(0, peers - 1, send, 0)

    def add(source, k):
        names = [source[k, pl.ds(CAP + c, 1), :] for c in range(CAP)]
        lines = [source[k, pl.ds(c, 1), :] for c in range(CAP)]
        block = lax.broadcasted_iota(jnp.int32, (BLK_SHARD, width), 0).astype(jnp.float32)
        total = tot[...]
        for c in range(CAP):
            total = total + jnp.where(block == names[c], lines[c], jnp.float32(0.0))
        tot[...] = total

        def some(j, carry):
            at = pl.multiple_of(j * CHUNK, CHUNK)
            value = [acc[at + t] for t in range(CHUNK)]
            for c in range(CAP):
                held = source[k, pl.ds(META + c * prow, prow), :]
                name = jnp.broadcast_to(names[c], (prow, width))
                for t in range(CHUNK):
                    hot = name == (at + t).astype(jnp.float32)
                    value[t] = value[t] + jnp.where(hot, held, jnp.float32(0.0))
            for t in range(CHUNK):
                acc[at + t] = value[t]
            return carry

        lax.fori_loop(0, BLK_SHARD // CHUNK, some, 0)

    add(stg, 0)

    def take(k):
        message(k).wait_recv()
        add(recv, k)

    def near(k, carry):
        take(k)
        return carry

    def far(i, carry):
        take(peers - 1 - i)
        return carry

    lax.fori_loop(1, peers // 2, near, 0)
    lax.fori_loop(0, peers - peers // 2, far, 0)

    def sent(k, carry):
        message(k).wait_send()
        return carry

    lax.fori_loop(1, peers, sent, 0)

    invt[...] = (jnp.float32(1.0) / jnp.maximum(tot[...], jnp.float32(1.0))).T
    inv = invt[pl.ds(pl.multiple_of(rep * prow, prow), prow), :]
    square = jnp.zeros((prow, width), jnp.float32)
    for t in range(BLK_SHARD):
        mean = acc[t] * inv[:, t : t + 1]
        acc[t] = mean
        square = square + mean * mean
    part[...] = jnp.sum(square.reshape(prow // 8, 8, width), axis=0)

    def norm(k):
        return pltpu.make_async_remote_copy(
            src_ref=part,
            dst_ref=norms.at[k],
            send_sem=nsend_sem.at[k],
            recv_sem=nrecv_sem.at[k],
            device_id=peer(k),
            device_id_type=pl.DeviceIdType.MESH,
        )

    def nsend(i, carry):
        norm(peers - 1 - i).start()
        return carry

    lax.fori_loop(0, peers - 1, nsend, 0)

    def ntake(k, total):
        norm(k).wait_recv()
        return total + norms[k]

    total = lax.fori_loop(1, peers, ntake, part[...])
    norm2 = jnp.sum(jnp.sum(total, axis=0, keepdims=True), axis=1, keepdims=True)
    scale = jnp.minimum(jnp.float32(1.0), limit / jnp.sqrt(norm2 + jnp.float32(1e-06)))
    for t in range(BLK_SHARD):
        out_ref[t] = acc[t] * scale

    def nsent(k, carry):
        norm(k).wait_send()
        return carry

    lax.fori_loop(1, peers, nsent, 0)


def local(nrep, nshard, grads, counts, block_owner, block_local):
    nblocks, rows, width = grads.shape[2:]
    peers = nrep * nshard
    prow = rows // nrep
    limit = math.sqrt(BLK_SHARD * nshard * rows * width) * 0.2
    body = functools.partial(kernel, nrep, nshard, limit)
    smem = pl.BlockSpec(memory_space=pltpu.SMEM)
    vmem = pl.BlockSpec(memory_space=pltpu.VMEM)
    size = META + CAP * prow
    return pl.pallas_call(
        body,
        out_shape=jax.ShapeDtypeStruct((BLK_SHARD, prow, width), jnp.float32),
        in_specs=[smem, smem, vmem, vmem],
        out_specs=vmem,
        scratch_shapes=[
            pltpu.VMEM((nblocks, rows, width), jnp.float32),
            pltpu.VMEM((peers, size, width), jnp.float32),
            pltpu.VMEM((peers, size, width), jnp.float32),
            pltpu.VMEM((BLK_SHARD, prow, width), jnp.float32),
            pltpu.VMEM((BLK_SHARD, width), jnp.float32),
            pltpu.VMEM((width, BLK_SHARD), jnp.float32),
            pltpu.VMEM((8, width), jnp.float32),
            pltpu.VMEM((peers, 8, width), jnp.float32),
            pltpu.SemaphoreType.DMA((peers,)),
            pltpu.SemaphoreType.DMA((peers,)),
            pltpu.SemaphoreType.DMA((peers,)),
            pltpu.SemaphoreType.DMA((peers,)),
        ],
        compiler_params=pltpu.CompilerParams(collective_id=0, has_side_effects=True),
        name="exchange",
    )(
        block_owner.reshape(nblocks),
        block_local.reshape(nblocks),
        counts.reshape(nblocks, rows),
        grads.reshape(nblocks, rows, width),
    )


def solution(mesh):
    body = functools.partial(local, mesh.shape["rep"], mesh.shape["shard"])
    return jax.shard_map(
        body,
        mesh=mesh,
        in_specs=(
            P("rep", "shard", None, None, None),
            P("rep", "shard", None, None),
            P("rep", "shard", None, None),
            P("rep", "shard", None),
        ),
        out_specs=P("shard", "rep", None),
        check_vma=False,
    )
```
